32 devices in a mesh: seq: 16 (over z, x, core), head: 2 (over y).
Axes of the slice: x: 2, y: 2, z: 4, core: 2. Of those that a mesh axis runs over, the one named last changes fastest.
Arguments:
- hidden: bfloat16 [4608, 8192], P('seq'), may hold values from -6 to 6
- norm_gain: bfloat16 [8192], replicated, may hold values from 0.099609375 to 1.8984375
- w_query: bfloat16 [8192, 1024], P('seq', 'head'), may hold values from -0.125 to 0.125
- w_key: bfloat16 [8192, 256], P('seq', 'head'), may hold values from -0.125 to 0.125
- w_value: bfloat16 [8192, 256], P('seq', 'head'), may hold values from -0.0625 to 0.0625
- bias_query: bfloat16 [1024], P('head'), may hold values from -3 to 3
- bias_key: bfloat16 [256], P('head'), may hold values from -200 to 200
- bias_value: bfloat16 [256], P('head'), may hold values from -3 to 3
- w_out: bfloat16 [1024, 8192], P('head', 'seq'), may hold values from -0.1875 to 0.1875
Outputs:
- attn_out: bfloat16 [4608, 8192], P(('seq', 'head'))
The draws below stay inside these ranges and needn't reach their ends.
All inputs are finite; a program needn't handle non-finite values.
Results may differ from the reference program's by a relative error of at most 0.014.
The reference program's roundings to bfloat16 on the way count: a program that leaves them out, or rounds other values in their place, can miss the bound.
Values may be sent and summed in bfloat16 or wider, within the bound.
A program may use at most 192 MiB of HBM per device.

```python
import jax
import jax.numpy as jnp
from jax import lax

D = 8192
HEAD_DIM = 128
QPG = 4
KV_HEADS = 2
LENGTH = 4608


def draw_bias_key(key, part):
    count = KV_HEADS * HEAD_DIM
    base = jax.random.normal(key, (count,), jnp.float32)
    return jnp.clip(0.5 * base, -3.0, 3.0).astype(jnp.bfloat16)


def steps_of(own_key, extent, split, least, high):
    gain = 1.0
    for position, shards_of in split:
        heights = jax.random.uniform(jax.random.fold_in(jax.random.fold_in(own_key, 6), position), (shards_of,), jnp.float32, least / len(split), high / len(split))
        gain = gain * jnp.repeat(jnp.exp(heights), extent[position] // shards_of).reshape((-1,) + (1,) * (len(extent) - 1 - position))
    return gain


def noise(own_key, dims, deviation, limit, split=(), kind=jnp.bfloat16):
    values = deviation * jax.random.normal(own_key, dims, jnp.float32)
    if split:
        values = values * steps_of(own_key, dims, split, -0.22, 0.18)
    return jnp.clip(values, -limit, limit).astype(kind)


def setup_inputs(seed: int = 0) -> dict:
    key_of = jax.random.split(jax.random.key(seed), 10)
    hidden = noise(key_of[0], (LENGTH, D), 1.0, 6.0, ((0, 16),))
    norm_gain = jnp.clip(1.0 + 0.18 * jax.random.normal(key_of[1], (D,), jnp.float32), 0.099609375, 1.8984375).astype(jnp.bfloat16)
    w_query = noise(key_of[2], (D, KV_HEADS * QPG * HEAD_DIM), (D // 4) ** -0.5, 0.125, ((0, 16), (1, 2)))
    w_key = noise(key_of[3], (D, KV_HEADS * HEAD_DIM), (D // 4) ** -0.5, 0.125, ((0, 16), (1, 2)))
    w_value = noise(key_of[4], (D, KV_HEADS * HEAD_DIM), D ** -0.5, 0.0625, ((0, 16), (1, 2)))
    bias_query = noise(key_of[5], (KV_HEADS * QPG * HEAD_DIM,), 0.5, 3.0, ((0, 2),))
    bias_key = draw_bias_key(jax.random.fold_in(key_of[9], 71), 0)
    bias_value = noise(key_of[7], (KV_HEADS * HEAD_DIM,), 0.5, 3.0, ((0, 2),))
    w_out = noise(key_of[8], (KV_HEADS * QPG * HEAD_DIM, D), (KV_HEADS * QPG * HEAD_DIM) ** -0.5, 0.1875, ((0, 2), (1, 16)))
    return dict(hidden=hidden, norm_gain=norm_gain, w_query=w_query, w_key=w_key, w_value=w_value, bias_query=bias_query, bias_key=bias_key, bias_value=bias_value, w_out=w_out)


ROPE_BASE = 1000000.0
EPSILON = 1e-06

def rotary(values, positions):
    half = values.shape[-1] // 2
    freq = ROPE_BASE ** (-2.0 * jnp.arange(half, dtype=jnp.float32) / values.shape[-1])
    angles = positions.astype(jnp.float32)[:, None, None] * freq[None, None, :]
    cosine = jnp.cos(angles)
    sine = jnp.sin(angles)
    first = values[..., :half]
    second = values[..., half:]
    return jnp.concatenate([first * cosine - second * sine, second * cosine + first * sine], axis=-1)

def reference(hidden, norm_gain, w_query, w_key, w_value, bias_query, bias_key, bias_value, w_out):
    length = hidden.shape[0]
    widened = hidden.astype(jnp.float32)
    inverse = lax.rsqrt(lax.optimization_barrier(jnp.mean(widened * widened, axis=-1, keepdims=True)) + EPSILON)
    normed = (widened * inverse * norm_gain.astype(jnp.float32)).astype(jnp.bfloat16)
    positions = jnp.arange(length, dtype=jnp.int32)
    query = jnp.dot(normed, w_query, preferred_element_type=jnp.float32) + bias_query.astype(jnp.float32)
    keys = jnp.dot(normed, w_key, preferred_element_type=jnp.float32) + bias_key.astype(jnp.float32)
    values = jnp.dot(normed, w_value, preferred_element_type=jnp.float32) + bias_value.astype(jnp.float32)
    query = rotary(query.reshape(length, KV_HEADS * QPG, HEAD_DIM), positions).astype(jnp.bfloat16)
    keys = rotary(keys.reshape(length, KV_HEADS, HEAD_DIM), positions).astype(jnp.bfloat16)
    values = values.reshape(length, KV_HEADS, HEAD_DIM).astype(jnp.bfloat16)
    query_groups = query.reshape(length, KV_HEADS, QPG, HEAD_DIM).transpose(1, 2, 0, 3)
    key_groups = keys.transpose(1, 0, 2)
    value_groups = values.transpose(1, 0, 2)
    causal = positions[:, None] >= positions[None, :]
    out_groups = w_out.reshape(KV_HEADS, QPG * HEAD_DIM, w_out.shape[1])

    def attend(carry, group):
        group_query, group_key, group_value, group_out = group
        scores = jnp.einsum('hqd,kd->hqk', group_query.astype(jnp.float32), group_key.astype(jnp.float32)) * HEAD_DIM ** (-0.5)
        scores = jnp.where(causal[None], scores, -jnp.inf)
        highest = lax.optimization_barrier(jnp.max(scores, axis=-1, keepdims=True))
        probs = jnp.exp(scores - highest)
        total = lax.optimization_barrier(jnp.sum(probs, axis=-1, keepdims=True))
        rounded = lax.optimization_barrier(probs.astype(jnp.bfloat16))
        mixed = jnp.einsum('hqk,kd->hqd', rounded.astype(jnp.float32), group_value.astype(jnp.float32))
        attended = (mixed / total).astype(jnp.bfloat16)
        attended = attended.transpose(1, 0, 2).reshape(length, QPG * HEAD_DIM)
        term = jnp.dot(attended, group_out, preferred_element_type=jnp.float32)
        term = lax.optimization_barrier(term.astype(jnp.bfloat16))
        return (carry + term.astype(jnp.float32), None)
    start = jnp.zeros((length, w_out.shape[1]), jnp.float32)
    summed, unused = lax.scan(attend, start, (query_groups, key_groups, value_groups, out_groups))
    return summed.astype(jnp.bfloat16)
```

```python
import functools

import jax
import jax.numpy as jnp
from jax import lax
from jax.experimental import pallas as pl
from jax.experimental.pallas import tpu as pltpu
from jax.sharding import PartitionSpec as P

HEAD_DIM = 128
ROPE_BASE = 1000000.0
EPSILON = 1e-06
MESH = pl.DeviceIdType.MESH
F32 = jnp.float32
BF16 = jnp.bfloat16


def kernel(
    n, groups, exchange,
    hidden, w_query, w_key, w_value, w_out, gain, bias, cosine, sine,
    out,
    hid, normed, w_all, wo_all, acc, kv_all, q_ref, high, total, mixed, att, ts, tr, tm,
    load_sem, ws, wr, wps, wpr, os_, or_, ops, opr, ks, kr, kps, kpr, ys, yr,
):
    chips = n // 2
    depth = chips // 2
    me = lax.axis_index("seq")
    group = lax.axis_index("head")
    core = me % 2
    chip = me // 2
    ring = chip // 2 + (chip % 2) * (2 * depth - 1 - 2 * (chip // 2))

    def device_at(position, which):
        position = (position + 2 * chips) % chips
        side = position // depth
        row = position + side * (2 * depth - 1 - 2 * position)
        return 2 * (2 * row + side) + which

    right = device_at(ring + 1, core)
    left = device_at(ring - 1, core)
    partner = 2 * chip + (1 - core)
    neighbours = (right, left)

    def source_at(direction, offset, which):
        return device_at(ring - offset if direction == 0 else ring + offset, which)

    rows, width = hidden.shape
    half_depth = w_query.shape[0] // 2
    q_cols = w_query.shape[1]
    heads = q_cols // HEAD_DIM
    half_cols = w_out.shape[1] // 2
    rh = rows // groups

    loads = [pltpu.make_async_copy(hidden, hid, load_sem.at[0])]
    for h in range(2):
        span = pl.ds(h * half_depth, half_depth)
        slot = w_all.at[2 * me + h]
        loads.append(pltpu.make_async_copy(w_query.at[span], slot.at[:, pl.ds(0, q_cols)], load_sem.at[1 + 4 * h]))
        loads.append(pltpu.make_async_copy(w_key.at[span], slot.at[:, pl.ds(q_cols, HEAD_DIM)], load_sem.at[2 + 4 * h]))
        loads.append(pltpu.make_async_copy(w_value.at[span], slot.at[:, pl.ds(q_cols + HEAD_DIM, HEAD_DIM)], load_sem.at[3 + 4 * h]))
        loads.append(pltpu.make_async_copy(w_out.at[:, pl.ds(h * half_cols, half_cols)], wo_all.at[2 * me + h], load_sem.at[4 + 4 * h]))
    for copy in loads:
        copy.start()

    barrier = pltpu.get_barrier_semaphore()
    for device in (right, left, partner):
        pl.semaphore_signal(barrier, inc=1, device_id={"seq": device}, device_id_type=MESH)
    peers = range(1, groups) if exchange else ()
    for p in peers:
        pl.semaphore_signal(barrier, inc=1, device_id={"head": (group + p) % groups}, device_id_type=MESH)
    pl.semaphore_wait(barrier, 3 + len(peers))

    def remote(ref, send, recv, key, device):
        return pltpu.make_async_remote_copy(
            src_ref=ref, dst_ref=ref, send_sem=send.at[key], recv_sem=recv.at[key],
            device_id={"seq": device}, device_id_type=MESH,
        )

    def piece(buffer, index, j):
        size = buffer.shape[1] // 2
        return buffer.at[index, pl.ds(j * size, size)]

    def key_of(direction, step, j):
        return (direction * chips + step) * 2 + j

    def ring_begin(buffer, sems):
        ss, rs, pss, prs = sems
        for j in range(2):
            for d in range(2):
                own = piece(buffer, 2 * me + d, j)
                remote(own, ss, rs, key_of(d, 0, j), neighbours[d]).start()
        for j in range(2):
            for d in range(2):
                own = piece(buffer, 2 * me + d, j)
                remote(own, pss, prs, key_of(d, chips - 1, j), partner).start()

    def ring_advance(buffer, sems, t):
        ss, rs, pss, prs = sems

        @pl.when(t < chips - 1)
        def _():
            for j in range(2):
                for d in range(2):
                    block = piece(buffer, 2 * source_at(d, t + 1, core) + d, j)
                    remote(block, ss, rs, key_of(d, t, j), neighbours[d]).wait_recv()

                    @pl.when(t < chips - 2)
                    def _():
                        remote(block, ss, rs, key_of(d, t + 1, j), neighbours[d]).start()

                    remote(block, pss, prs, key_of(d, t, j), partner).start()

    def partner_wait(buffer, sems, t):
        ss, rs, pss, prs = sems
        for j in range(2):
            for d in range(2):
                block = piece(buffer, 2 * source_at(d, t, 1 - core) + d, j)
                remote(block, pss, prs, key_of(d, (t + chips - 1) % chips, j), partner).wait_recv()

    def ring_drain(buffer, sems):
        ss, rs, pss, prs = sems

        def body(t, carry):
            for j in range(2):
                for d in range(2):
                    block = piece(buffer, 2 * me + d, j)

                    @pl.when(t < chips - 1)
                    def _():
                        remote(block, ss, rs, key_of(d, t, j), neighbours[d]).wait_send()

                    remote(block, pss, prs, key_of(d, t, j), partner).wait_send()
            return carry

        lax.fori_loop(0, chips, body, 0)

    w_sems = (ws, wr, wps, wpr)
    o_sems = (os_, or_, ops, opr)

    for copy in loads[1:]:
        copy.wait()
    ring_begin(w_all, w_sems)
    loads[0].wait()
    slices = 2 * n
    step_cols = width // slices

    def columns(i):
        return pl.ds(pl.multiple_of(i * step_cols, step_cols), step_cols)

    def square(i, carry):
        x = hid[:, columns(i)].astype(F32)
        return carry + x * x

    squares = lax.fori_loop(0, slices, square, jnp.zeros((rows, step_cols), F32))
    inverse = lax.rsqrt(jnp.sum(squares, axis=-1, keepdims=True) * (1.0 / width) + EPSILON)

    def normalise(i, carry):
        x = hid[:, columns(i)].astype(F32)
        normed[i] = (x * inverse * gain[i]).astype(BF16)
        return carry

    lax.fori_loop(0, slices, normalise, 0)
    acc[...] = jnp.broadcast_to(bias[...], acc.shape)

    def project(t, carry):
        ring_advance(w_all, w_sems, t)
        partner_wait(w_all, w_sems, t)
        for d in range(2):
            i = 2 * source_at(d, t, core) + d
            k = 2 * source_at(d, t, 1 - core) + d
            acc[...] += jnp.dot(normed[i], w_all[i], preferred_element_type=F32) + jnp.dot(
                normed[k], w_all[k], preferred_element_type=F32
            )
        return carry

    lax.fori_loop(0, chips, project, 0)

    def rotary(x):
        return x * cosine[...] + pltpu.roll(x, HEAD_DIM // 2, 1) * sine[...]

    kv_all[me, :, pl.ds(0, HEAD_DIM)] = rotary(acc[:, pl.ds(q_cols, HEAD_DIM)]).astype(BF16)
    kv_all[me, :, pl.ds(HEAD_DIM, HEAD_DIM)] = acc[:, pl.ds(q_cols + HEAD_DIM, HEAD_DIM)].astype(BF16)
    for h in range(heads):
        q_ref[h] = rotary(acc[:, pl.ds(h * HEAD_DIM, HEAD_DIM)]).astype(BF16)

    reach = (chips // 2, chips - 1 - chips // 2)

    def kv_copy(owner, ss, rs, direction, step, device):
        return remote(kv_all.at[owner], ss, rs, direction * chips + step, device)

    for d in range(2):
        kv_copy(me, ks, kr, d, 0, neighbours[d]).start()
    kv_copy(me, kps, kpr, 0, chips - 1, partner).start()

    scaling = HEAD_DIM ** (-0.5)

    def attend(b, first, diagonal):
        for h in range(heads):
            scores = lax.dot_general(
                q_ref[h], kv_all[b, :, pl.ds(0, HEAD_DIM)], (((1,), (1,)), ((), ())),
                preferred_element_type=F32,
            ) * scaling
            if diagonal:
                row = lax.broadcasted_iota(jnp.int32, scores.shape, 0)
                col = lax.broadcasted_iota(jnp.int32, scores.shape, 1)
                scores = jnp.where(row >= col, scores, -jnp.inf)
            top = jnp.max(scores, axis=-1, keepdims=True)
            if not first:
                old = high[h]
                top = jnp.maximum(old, top)
            probs = jnp.exp(scores - top)
            part = jnp.sum(probs, axis=-1, keepdims=True)
            product = jnp.dot(
                probs.astype(BF16), kv_all[b, :, pl.ds(HEAD_DIM, HEAD_DIM)], preferred_element_type=F32
            )
            if not first:
                shrink = jnp.exp(old - top)
                part = part + total[h] * shrink
                product = product + mixed[h] * shrink
            high[h] = top
            total[h] = part
            mixed[h] = product

    attend(me, True, True)

    def attend_earlier(b):
        @pl.when(b < me)
        def _():
            attend(b, False, False)

    def attention(t, carry):
        for d in range(2):
            @pl.when(t < reach[d])
            def _():
                owner = source_at(d, t + 1, core)
                kv_copy(owner, ks, kr, d, t, neighbours[d]).wait_recv()

                @pl.when(t + 1 < reach[d])
                def _():
                    kv_copy(owner, ks, kr, d, t + 1, neighbours[d]).start()

                kv_copy(owner, kps, kpr, d, t, partner).start()

        @pl.when(t == 0)
        def _():
            kv_copy(partner, kps, kpr, 0, chips - 1, partner).wait_recv()
            attend_earlier(partner)

        for d in range(2):
            @pl.when((t > 0) & (t <= reach[d]))
            def _():
                attend_earlier(source_at(d, t, core))
                owner = source_at(d, t, 1 - core)
                kv_copy(owner, kps, kpr, d, t - 1, partner).wait_recv()
                attend_earlier(owner)
        return carry

    lax.fori_loop(0, reach[0] + 1, attention, 0)
    ring_begin(wo_all, o_sems)
    for h in range(heads):
        att[:, pl.ds(h * HEAD_DIM, HEAD_DIM)] = (mixed[h] / total[h]).astype(BF16)

    def term_copy(p, i):
        return pltpu.make_async_remote_copy(
            src_ref=ts.at[p - 1, i], dst_ref=tr.at[p - 1, i],
            send_sem=ys.at[(p - 1) * slices + i], recv_sem=yr.at[(p - 1) * slices + i],
            device_id={"head": (group + p) % groups}, device_id_type=MESH,
        )

    def out_columns(i):
        return pl.ds(pl.multiple_of(i * half_cols, half_cols), half_cols)

    def make_term(i):
        if not exchange:
            out[:, out_columns(i)] = jnp.dot(att[...], wo_all[i], preferred_element_type=F32).astype(BF16)
            return
        for p in peers:
            span = pl.ds(pl.multiple_of(((group + p) % groups) * rh, rh), rh)
            ts[p - 1, i] = jnp.dot(att[span, :], wo_all[i], preferred_element_type=F32).astype(BF16)
            term_copy(p, i).start()
        span = pl.ds(pl.multiple_of(group * rh, rh), rh)
        tm[i] = jnp.dot(att[span, :], wo_all[i], preferred_element_type=F32).astype(BF16)

    def blocks_of(t):
        return [2 * source_at(d, t, which) + d for d in range(2) for which in (core, 1 - core)]

    def project_out(t, carry):
        ring_advance(wo_all, o_sems, t)
        partner_wait(wo_all, o_sems, t)
        for i in blocks_of(t):
            make_term(i)
        return carry

    lax.fori_loop(0, chips, project_out, 0)

    def finish(t, carry):
        for i in blocks_of(t):
            value = tm[i].astype(F32)
            for p in peers:
                term_copy(p, i).wait_recv()
                value = value + tr[p - 1, i].astype(F32)
            out[:, out_columns(i)] = value.astype(BF16)
        return carry

    if exchange:
        lax.fori_loop(0, chips, finish, 0)

        def sent(i, carry):
            for p in peers:
                term_copy(p, i).wait_send()
            return carry

        lax.fori_loop(0, slices, sent, 0)

    ring_drain(w_all, w_sems)
    ring_drain(wo_all, o_sems)
    for d in range(2):
        for t in range(reach[d]):
            kv_copy(me, ks, kr, d, t, neighbours[d]).wait_send()
            kv_copy(me, kps, kpr, d, t, partner).wait_send()
    kv_copy(me, kps, kpr, 0, chips - 1, partner).wait_send()


def local(n, groups, hidden, norm_gain, w_query, w_key, w_value, bias_query, bias_key, bias_value, w_out):
    rows, width = hidden.shape
    cols = w_query.shape[1]
    heads = cols // HEAD_DIM
    wide = cols + 2 * HEAD_DIM
    chips = n // 2
    exchange = groups > 1 and (rows // groups) % 16 == 0
    rh = rows // groups
    slices = 2 * n
    half_depth = w_query.shape[0] // 2
    half_cols = w_out.shape[1] // 2

    positions = lax.axis_index("seq") * rows + jnp.arange(rows, dtype=jnp.int32)
    freq = ROPE_BASE ** (-2.0 * jnp.arange(HEAD_DIM // 2, dtype=F32) / HEAD_DIM)
    angles = positions.astype(F32)[:, None] * freq[None, :]
    cosine = jnp.cos(angles)
    sine = jnp.sin(angles)
    cosine = jnp.concatenate([cosine, cosine], axis=-1)
    sine = jnp.concatenate([-sine, sine], axis=-1)
    gain = norm_gain.astype(F32).reshape(slices, 1, width // slices)
    bias = jnp.concatenate([bias_query, bias_key, bias_value]).astype(F32)[None, :]

    any_spec = pl.BlockSpec(memory_space=pl.ANY)
    vmem = pl.BlockSpec(memory_space=pltpu.VMEM)
    links = max(groups - 1, 1) if exchange else 1
    pieces = slices if exchange else 1
    rpart = rh if exchange else 16
    dma = pltpu.SemaphoreType.DMA
    result = pl.pallas_call(
        functools.partial(kernel, n, groups, exchange),
        out_shape=jax.ShapeDtypeStruct((rh if exchange else rows, w_out.shape[1] * n), BF16),
        in_specs=[any_spec] * 5 + [vmem] * 4,
        out_specs=vmem,
        scratch_shapes=[
            pltpu.VMEM((rows, width), BF16),
            pltpu.VMEM((slices, rows, width // slices), BF16),
            pltpu.VMEM((slices, half_depth, wide), BF16),
            pltpu.VMEM((slices, w_out.shape[0], half_cols), BF16),
            pltpu.VMEM((rows, wide), F32),
            pltpu.VMEM((n, rows, 2 * HEAD_DIM), BF16),
            pltpu.VMEM((heads, rows, HEAD_DIM), BF16),
            pltpu.VMEM((heads, rows, 1), F32),
            pltpu.VMEM((heads, rows, 1), F32),
            pltpu.VMEM((heads, rows, HEAD_DIM), F32),
            pltpu.VMEM((rows, cols), BF16),
            pltpu.VMEM((links, pieces, rpart, half_cols), BF16),
            pltpu.VMEM((links, pieces, rpart, half_cols), BF16),
            pltpu.VMEM((pieces, rpart, half_cols), BF16),
            dma((9,)),
        ]
        + [dma((4 * chips,))] * 8
        + [dma((2 * chips,))] * 4
        + [dma((links * pieces,))] * 2,
        compiler_params=pltpu.CompilerParams(
            collective_id=0, has_side_effects=True, vmem_limit_bytes=64 * 1024 * 1024 - 128 * 1024
        ),
    )(hidden, w_query, w_key, w_value, w_out, gain, bias, cosine, sine)
    if exchange:
        return result
    return lax.psum_scatter(result, "head", scatter_dimension=0, tiled=True)


def solution(mesh):
    in_specs = (
        P("seq", None),
        P(),
        P("seq", "head"),
        P("seq", "head"),
        P("seq", "head"),
        P("head"),
        P("head"),
        P("head"),
        P("head", "seq"),
    )
    out_specs = P(("seq", "head"), None)
    body = functools.partial(local, mesh.shape["seq"], mesh.shape["head"])
    return jax.shard_map(body, mesh=mesh, in_specs=in_specs, out_specs=out_specs, check_vma=False)
```

```python
import functools

import jax
import jax.numpy as jnp
import numpy as np
from jax import lax
from jax.experimental import pallas as pl
from jax.experimental.pallas import tpu as pltpu
from jax.sharding import PartitionSpec as P

HEAD_DIM = 128
ROPE_BASE = 1000000.0
EPSILON = 1e-06
MESH = pl.DeviceIdType.MESH
F32 = jnp.float32
BF16 = jnp.bfloat16


def kernel(
    n, groups, exchange,
    hidden, w_query, w_key, w_value, w_out, gain, bias_query, bias_key, bias_value,
    near_cos, near_sin, far_cos, far_sin,
    out,
    hid, w_all, wo_all, acc, kv_all, q_ref, high, total, mixed, att, ts, tr, tm,
    load_sem, ws, wr, wps, wpr, os_, or_, ops, opr, ks, kr, kps, kpr, ys, yr,
):
    chips = n // 2
    depth = chips // 2
    me = lax.axis_index("seq")
    group = lax.axis_index("head")
    core = me % 2
    chip = me // 2
    ring = chip // 2 + (chip % 2) * (2 * depth - 1 - 2 * (chip // 2))

    def device_at(position, which):
        position = (position + 2 * chips) % chips
        side = position // depth
        row = position + side * (2 * depth - 1 - 2 * position)
        return 2 * (2 * row + side) + which

    right = device_at(ring + 1, core)
    left = device_at(ring - 1, core)
    partner = 2 * chip + (1 - core)
    neighbours = (right, left)

    def source_at(direction, offset, which):
        return device_at(ring - offset if direction == 0 else ring + offset, which)

    rows, width = hidden.shape
    half_depth = w_query.shape[0] // 2
    q_cols = w_query.shape[1]
    heads = q_cols // HEAD_DIM
    half_cols = w_out.shape[1] // 2
    rh = rows // groups

    loads = [pltpu.make_async_copy(hidden, hid, load_sem.at[0])]
    for h in range(2):
        span = pl.ds(h * half_depth, half_depth)
        slot = w_all.at[2 * me + h]
        loads.append(pltpu.make_async_copy(w_query.at[span], slot.at[:, pl.ds(0, q_cols)], load_sem.at[1 + 4 * h]))
        loads.append(pltpu.make_async_copy(w_key.at[span], slot.at[:, pl.ds(q_cols, HEAD_DIM)], load_sem.at[2 + 4 * h]))
        loads.append(pltpu.make_async_copy(w_value.at[span], slot.at[:, pl.ds(q_cols + HEAD_DIM, HEAD_DIM)], load_sem.at[3 + 4 * h]))
        loads.append(pltpu.make_async_copy(w_out.at[:, pl.ds(h * half_cols, half_cols)], wo_all.at[2 * me + h], load_sem.at[4 + 4 * h]))
    for copy in loads:
        copy.start()

    barrier = pltpu.get_barrier_semaphore()
    for device in (right, left, partner):
        pl.semaphore_signal(barrier, inc=1, device_id={"seq": device}, device_id_type=MESH)
    peers = range(1, groups) if exchange else ()
    for p in peers:
        pl.semaphore_signal(barrier, inc=1, device_id={"head": (group + p) % groups}, device_id_type=MESH)
    pl.semaphore_wait(barrier, 3 + len(peers))

    def remote(ref, send, recv, key, device):
        return pltpu.make_async_remote_copy(
            src_ref=ref, dst_ref=ref, send_sem=send.at[key], recv_sem=recv.at[key],
            device_id={"seq": device}, device_id_type=MESH,
        )

    def piece(buffer, index, j):
        size = buffer.shape[1] // 2
        return buffer.at[index, pl.ds(j * size, size)]

    def key_of(direction, step, j):
        return (direction * chips + step) * 2 + j

    def ring_begin(buffer, sems):
        ss, rs, pss, prs = sems
        for j in range(2):
            for d in range(2):
                own = piece(buffer, 2 * me + d, j)
                remote(own, ss, rs, key_of(d, 0, j), neighbours[d]).start()
        for j in range(2):
            for d in range(2):
                own = piece(buffer, 2 * me + d, j)
                remote(own, pss, prs, key_of(d, chips - 1, j), partner).start()

    def ring_advance(buffer, sems, t):
        ss, rs, pss, prs = sems

        @pl.when(t < chips - 1)
        def _():
            for j in range(2):
                for d in range(2):
                    block = piece(buffer, 2 * source_at(d, t + 1, core) + d, j)
                    remote(block, ss, rs, key_of(d, t, j), neighbours[d]).wait_recv()

                    @pl.when(t < chips - 2)
                    def _():
                        remote(block, ss, rs, key_of(d, t + 1, j), neighbours[d]).start()

                    remote(block, pss, prs, key_of(d, t, j), partner).start()

    def partner_wait(buffer, sems, t):
        ss, rs, pss, prs = sems
        for j in range(2):
            for d in range(2):
                block = piece(buffer, 2 * source_at(d, t, 1 - core) + d, j)
                remote(block, pss, prs, key_of(d, (t + chips - 1) % chips, j), partner).wait_recv()

    def ring_drain(buffer, sems):
        ss, rs, pss, prs = sems

        def body(t, carry):
            for j in range(2):
                for d in range(2):
                    block = piece(buffer, 2 * me + d, j)

                    @pl.when(t < chips - 1)
                    def _():
                        remote(block, ss, rs, key_of(d, t, j), neighbours[d]).wait_send()

                    remote(block, pss, prs, key_of(d, t, j), partner).wait_send()
            return carry

        lax.fori_loop(0, chips, body, 0)

    w_sems = (ws, wr, wps, wpr)
    o_sems = (os_, or_, ops, opr)

    for copy in loads[1:]:
        copy.wait()
    ring_begin(w_all, w_sems)
    loads[0].wait()
    slices = 2 * n
    step_cols = width // slices

    def columns(i):
        return pl.ds(pl.multiple_of(i * step_cols, step_cols), step_cols)

    def square(i, carry):
        x = hid[:, columns(i)].astype(F32)
        return carry + x * x

    squares = lax.fori_loop(0, slices, square, jnp.zeros((rows, step_cols), F32))
    inverse = lax.rsqrt(jnp.sum(squares, axis=-1, keepdims=True) * (1.0 / width) + EPSILON)

    def normed(i):
        scaled = hid[:, columns(i)].astype(F32) * inverse * gain[:, columns(i)].astype(F32)
        return scaled.astype(BF16)

    bias = (bias_query, bias_key, bias_value)
    starts = (0, q_cols, q_cols + HEAD_DIM)
    for start, part in zip(starts, bias):
        span = pl.ds(start, part.shape[1])
        acc[:, span] = jnp.broadcast_to(part[...].astype(F32), (rows, part.shape[1]))

    def project(t, carry):
        ring_advance(w_all, w_sems, t)
        partner_wait(w_all, w_sems, t)
        for d in range(2):
            i = 2 * source_at(d, t, core) + d
            k = 2 * source_at(d, t, 1 - core) + d
            acc[...] += jnp.dot(normed(i), w_all[i], preferred_element_type=F32) + jnp.dot(
                normed(k), w_all[k], preferred_element_type=F32
            )
        return carry

    lax.fori_loop(0, chips, project, 0)

    block_cos, block_sin = far_cos[me], far_sin[me]
    cosine = near_cos[...] * block_cos - near_sin[...] * block_sin
    lane = lax.broadcasted_iota(jnp.int32, cosine.shape, 1)
    sine = near_sin[...] * block_cos + near_cos[...] * block_sin
    sine = jnp.where(lane < HEAD_DIM // 2, -sine, sine)

    def rotary(x):
        return x * cosine + pltpu.roll(x, HEAD_DIM // 2, 1) * sine

    def kv_rows(which):
        return pl.ds(pl.multiple_of(which * rows, rows), rows)

    kv_all[chip, kv_rows(core), pl.ds(0, HEAD_DIM)] = rotary(acc[:, pl.ds(q_cols, HEAD_DIM)]).astype(BF16)
    kv_all[chip, kv_rows(core), pl.ds(HEAD_DIM, HEAD_DIM)] = acc[:, pl.ds(q_cols + HEAD_DIM, HEAD_DIM)].astype(BF16)
    for h in range(heads):
        q_ref[h] = rotary(acc[:, pl.ds(h * HEAD_DIM, HEAD_DIM)]).astype(BF16)

    reach = (chips // 2, chips - 1 - chips // 2)

    def kv_copy(owner, ss, rs, direction, step, device):
        return remote(kv_all.at[owner // 2, kv_rows(owner % 2)], ss, rs, direction * chips + step, device)

    for d in range(2):
        kv_copy(me, ks, kr, d, 0, neighbours[d]).start()
    kv_copy(me, kps, kpr, 0, chips - 1, partner).start()

    factor = HEAD_DIM ** (-0.5) * 1.4426950408889634

    def attend(c, own):
        for h in range(heads):
            scores = lax.dot_general(
                q_ref[h], kv_all[c, :, pl.ds(0, HEAD_DIM)], (((1,), (1,)), ((), ())),
                preferred_element_type=F32,
            )
            if own:
                row = lax.broadcasted_iota(jnp.int32, scores.shape, 0) + core * rows
                col = lax.broadcasted_iota(jnp.int32, scores.shape, 1)
                scores = jnp.where(row >= col, scores, -jnp.inf)
            top = jnp.max(scores, axis=-1, keepdims=True)
            if not own:
                old = high[h]
                top = jnp.maximum(old, top)
            probs = jnp.exp2((scores - top) * factor)
            part = jnp.sum(probs, axis=-1, keepdims=True)
            product = jnp.dot(
                probs.astype(BF16), kv_all[c, :, pl.ds(HEAD_DIM, HEAD_DIM)], preferred_element_type=F32
            )
            if not own:
                shrink = jnp.exp2((old - top) * factor)
                part = part + total[h] * shrink
                product = product + mixed[h] * shrink
            high[h] = top
            total[h] = part
            mixed[h] = product

    kv_copy(partner, kps, kpr, 0, chips - 1, partner).wait_recv()
    attend(chip, True)

    def attention(t, carry):
        for d in range(2):
            @pl.when(t < reach[d])
            def _():
                owner = source_at(d, t + 1, core)
                kv_copy(owner, ks, kr, d, t, neighbours[d]).wait_recv()

                @pl.when(t + 1 < reach[d])
                def _():
                    kv_copy(owner, ks, kr, d, t + 1, neighbours[d]).start()

                kv_copy(owner, kps, kpr, d, t, partner).start()

        @pl.when(t == reach[0])
        def _():
            ring_begin(wo_all, o_sems)

        for d in range(2):
            @pl.when((t > 0) & (t <= reach[d]))
            def _():
                owner = source_at(d, t, 1 - core)
                kv_copy(owner, kps, kpr, d, t - 1, partner).wait_recv()

                @pl.when(owner // 2 < chip)
                def _():
                    attend(owner // 2, False)
        return carry

    lax.fori_loop(0, reach[0] + 1, attention, 0)
    for h in range(heads):
        att[:, pl.ds(h * HEAD_DIM, HEAD_DIM)] = (mixed[h] / total[h]).astype(BF16)

    def term_copy(p, i):
        return pltpu.make_async_remote_copy(
            src_ref=ts.at[p - 1, i], dst_ref=tr.at[p - 1, i],
            send_sem=ys.at[(p - 1) * slices + i], recv_sem=yr.at[(p - 1) * slices + i],
            device_id={"head": (group + p) % groups}, device_id_type=MESH,
        )

    def out_columns(i):
        return pl.ds(pl.multiple_of(i * half_cols, half_cols), half_cols)

    def make_term(i):
        if not exchange:
            out[:, out_columns(i)] = jnp.dot(att[...], wo_all[i], preferred_element_type=F32).astype(BF16)
            return
        for p in peers:
            span = pl.ds(pl.multiple_of(((group + p) % groups) * rh, rh), rh)
            ts[p - 1, i] = jnp.dot(att[span, :], wo_all[i], preferred_element_type=F32).astype(BF16)
            term_copy(p, i).start()
        span = pl.ds(pl.multiple_of(group * rh, rh), rh)
        tm[i] = jnp.dot(att[span, :], wo_all[i], preferred_element_type=F32).astype(BF16)

    def blocks_of(t):
        return [2 * source_at(d, t, which) + d for d in range(2) for which in (core, 1 - core)]

    def finish(t, carry):
        for i in blocks_of(t):
            value = tm[i].astype(F32)
            for p in peers:
                term_copy(p, i).wait_recv()
                value = value + tr[p - 1, i].astype(F32)
            out[:, out_columns(i)] = value.astype(BF16)
        return carry

    lag = 3

    def project_out(t, carry):
        ring_advance(wo_all, o_sems, t)
        partner_wait(wo_all, o_sems, t)
        for i in blocks_of(t):
            make_term(i)
        if exchange:
            @pl.when(t >= lag)
            def _():
                finish(t - lag, 0)
        return carry

    lax.fori_loop(0, chips, project_out, 0)

    if exchange:
        lax.fori_loop(chips - lag, chips, finish, 0)

        def sent(i, carry):
            for p in peers:
                term_copy(p, i).wait_send()
            return carry

        lax.fori_loop(0, slices, sent, 0)

    ring_drain(w_all, w_sems)
    ring_drain(wo_all, o_sems)
    for d in range(2):
        for t in range(reach[d]):
            kv_copy(me, ks, kr, d, t, neighbours[d]).wait_send()
            kv_copy(me, kps, kpr, d, t, partner).wait_send()
    kv_copy(me, kps, kpr, 0, chips - 1, partner).wait_send()


def local(n, groups, hidden, norm_gain, w_query, w_key, w_value, bias_query, bias_key, bias_value, w_out):
    rows, width = hidden.shape
    cols = w_query.shape[1]
    heads = cols // HEAD_DIM
    wide = cols + 2 * HEAD_DIM
    chips = n // 2
    exchange = groups > 1 and (rows // groups) % 16 == 0
    rh = rows // groups
    slices = 2 * n
    half_depth = w_query.shape[0] // 2
    half_cols = w_out.shape[1] // 2

    freq = ROPE_BASE ** (-2.0 * np.arange(HEAD_DIM // 2, dtype=np.float64) / HEAD_DIM)
    freq = np.concatenate([freq, freq])
    near = np.arange(rows, dtype=np.float64)[:, None] * freq
    far = (np.arange(n, dtype=np.float64) * rows)[:, None, None] * freq
    tables = [f(a).astype(np.float32) for a in (near, far) for f in (np.cos, np.sin)]
    vectors = [v.reshape(1, -1) for v in (norm_gain, bias_query, bias_key, bias_value)]

    any_spec = pl.BlockSpec(memory_space=pl.ANY)
    vmem = pl.BlockSpec(memory_space=pltpu.VMEM)
    links = max(groups - 1, 1) if exchange else 1
    pieces = slices if exchange else 1
    rpart = rh if exchange else 16
    dma = pltpu.SemaphoreType.DMA
    result = pl.pallas_call(
        functools.partial(kernel, n, groups, exchange),
        out_shape=jax.ShapeDtypeStruct((rh if exchange else rows, w_out.shape[1] * n), BF16),
        in_specs=[any_spec] * 5 + [vmem] * 8,
        out_specs=vmem,
        scratch_shapes=[
            pltpu.VMEM((rows, width), BF16),
            pltpu.VMEM((slices, half_depth, wide), BF16),
            pltpu.VMEM((slices, w_out.shape[0], half_cols), BF16),
            pltpu.VMEM((rows, wide), F32),
            pltpu.VMEM((chips, 2 * rows, 2 * HEAD_DIM), BF16),
            pltpu.VMEM((heads, rows, HEAD_DIM), BF16),
            pltpu.VMEM((heads, rows, 1), F32),
            pltpu.VMEM((heads, rows, 1), F32),
            pltpu.VMEM((heads, rows, HEAD_DIM), F32),
            pltpu.VMEM((rows, cols), BF16),
            pltpu.VMEM((links, pieces, rpart, half_cols), BF16),
            pltpu.VMEM((links, pieces, rpart, half_cols), BF16),
            pltpu.VMEM((pieces, rpart, half_cols), BF16),
            dma((9,)),
        ]
        + [dma((4 * chips,))] * 8
        + [dma((2 * chips,))] * 4
        + [dma((links * pieces,))] * 2,
        compiler_params=pltpu.CompilerParams(
            collective_id=0, has_side_effects=True, vmem_limit_bytes=64 * 1024 * 1024 - 128 * 1024
        ),
    )(hidden, w_query, w_key, w_value, w_out, *vectors, *tables)
    if exchange:
        return result
    return lax.psum_scatter(result, "head", scatter_dimension=0, tiled=True)


def solution(mesh):
    in_specs = (
        P("seq", None),
        P(),
        P("seq", "head"),
        P("seq", "head"),
        P("seq", "head"),
        P("head"),
        P("head"),
        P("head"),
        P("head", "seq"),
    )
    out_specs = P(("seq", "head"), None)
    body = functools.partial(local, mesh.shape["seq"], mesh.shape["head"])
    return jax.shard_map(body, mesh=mesh, in_specs=in_specs, out_specs=out_specs, check_vma=False)
```

```python
import functools

import jax
import jax.numpy as jnp
import numpy as np
from jax import lax
from jax.experimental import pallas as pl
from jax.experimental.pallas import tpu as pltpu
from jax.sharding import PartitionSpec as P

HEAD_DIM = 128
ROPE_BASE = 1000000.0
EPSILON = 1e-06
MESH = pl.DeviceIdType.MESH
F32 = jnp.float32
BF16 = jnp.bfloat16


def kernel(
    n, groups, exchange,
    hidden, w_query, w_key, w_value, w_out, gain, bias_query, bias_key, bias_value,
    near_cos, near_sin, far_cos, far_sin,
    out,
    hid, w_all, wo_all, acc, kv_all, q_ref, high, total, mixed, att, ts, tr, tm,
    load_sem, ws, wr, wps, wpr, os_, or_, ops, opr, ks, kr, kps, kpr, ys, yr,
):
    chips = n // 2
    depth = chips // 2
    me = lax.axis_index("seq")
    group = lax.axis_index("head")
    core = me % 2
    chip = me // 2
    ring = chip // 2 + (chip % 2) * (2 * depth - 1 - 2 * (chip // 2))

    def device_at(position, which):
        position = (position + 2 * chips) % chips
        side = position // depth
        row = position + side * (2 * depth - 1 - 2 * position)
        return 2 * (2 * row + side) + which

    right = device_at(ring + 1, core)
    left = device_at(ring - 1, core)
    partner = 2 * chip + (1 - core)
    neighbours = (right, left)

    def source_at(direction, offset, which):
        return device_at(ring - offset if direction == 0 else ring + offset, which)

    rows, width = hidden.shape
    half_depth = w_query.shape[0] // 2
    q_cols = w_query.shape[1]
    heads = q_cols // HEAD_DIM
    half_cols = w_out.shape[1] // 2
    rh = rows // groups

    loads = []
    late = [pltpu.make_async_copy(hidden, hid, load_sem.at[0])]
    for h in range(2):
        span = pl.ds(h * half_depth, half_depth)
        slot = w_all.at[2 * me + h]
        loads.append(pltpu.make_async_copy(w_query.at[span], slot.at[:, pl.ds(0, q_cols)], load_sem.at[1 + 4 * h]))
        loads.append(pltpu.make_async_copy(w_key.at[span], slot.at[:, pl.ds(q_cols, HEAD_DIM)], load_sem.at[2 + 4 * h]))
        loads.append(pltpu.make_async_copy(w_value.at[span], slot.at[:, pl.ds(q_cols + HEAD_DIM, HEAD_DIM)], load_sem.at[3 + 4 * h]))
        late.append(pltpu.make_async_copy(w_out.at[:, pl.ds(h * half_cols, half_cols)], wo_all.at[2 * me + h], load_sem.at[4 + 4 * h]))
    for copy in loads + late:
        copy.start()

    barrier = pltpu.get_barrier_semaphore()
    for device in (right, left, partner):
        pl.semaphore_signal(barrier, inc=1, device_id={"seq": device}, device_id_type=MESH)
    peers = range(1, groups) if exchange else ()
    for p in peers:
        pl.semaphore_signal(barrier, inc=1, device_id={"head": (group + p) % groups}, device_id_type=MESH)
    pl.semaphore_wait(barrier, 3 + len(peers))

    def remote(ref, send, recv, key, device):
        return pltpu.make_async_remote_copy(
            src_ref=ref, dst_ref=ref, send_sem=send.at[key], recv_sem=recv.at[key],
            device_id={"seq": device}, device_id_type=MESH,
        )

    def piece(buffer, index, j):
        size = buffer.shape[1] // 2
        return buffer.at[index, pl.ds(j * size, size)]

    def key_of(direction, step, j):
        return (direction * chips + step) * 2 + j

    def ring_begin(buffer, sems):
        ss, rs, pss, prs = sems
        for j in range(2):
            for d in range(2):
                own = piece(buffer, 2 * me + d, j)
                remote(own, ss, rs, key_of(d, 0, j), neighbours[d]).start()
        for j in range(2):
            for d in range(2):
                own = piece(buffer, 2 * me + d, j)
                remote(own, pss, prs, key_of(d, chips - 1, j), partner).start()

    def ring_advance(buffer, sems, t):
        ss, rs, pss, prs = sems

        @pl.when(t < chips - 1)
        def _():
            for j in range(2):
                for d in range(2):
                    block = piece(buffer, 2 * source_at(d, t + 1, core) + d, j)
                    remote(block, ss, rs, key_of(d, t, j), neighbours[d]).wait_recv()

                    @pl.when(t < chips - 2)
                    def _():
                        remote(block, ss, rs, key_of(d, t + 1, j), neighbours[d]).start()

                    remote(block, pss, prs, key_of(d, t, j), partner).start()

    def partner_wait(buffer, sems, t):
        ss, rs, pss, prs = sems
        for j in range(2):
            for d in range(2):
                block = piece(buffer, 2 * source_at(d, t, 1 - core) + d, j)
                remote(block, pss, prs, key_of(d, (t + chips - 1) % chips, j), partner).wait_recv()

    def ring_drain(buffer, sems):
        ss, rs, pss, prs = sems

        def body(t, carry):
            for j in range(2):
                for d in range(2):
                    block = piece(buffer, 2 * me + d, j)

                    @pl.when(t < chips - 1)
                    def _():
                        remote(block, ss, rs, key_of(d, t, j), neighbours[d]).wait_send()

                    remote(block, pss, prs, key_of(d, t, j), partner).wait_send()
            return carry

        lax.fori_loop(0, chips, body, 0)

    w_sems = (ws, wr, wps, wpr)
    o_sems = (os_, or_, ops, opr)

    for copy in loads:
        copy.wait()
    ring_begin(w_all, w_sems)
    for copy in late:
        copy.wait()
    slices = 2 * n
    step_cols = width // slices

    def columns(i):
        return pl.ds(pl.multiple_of(i * step_cols, step_cols), step_cols)

    def square(i, carry):
        x = hid[:, columns(i)].astype(F32)
        return carry + x * x

    squares = lax.fori_loop(0, slices, square, jnp.zeros((rows, step_cols), F32))
    inverse = lax.rsqrt(jnp.sum(squares, axis=-1, keepdims=True) * (1.0 / width) + EPSILON)

    def normed(i):
        scaled = hid[:, columns(i)].astype(F32) * inverse * gain[:, columns(i)].astype(F32)
        return scaled.astype(BF16)

    bias = (bias_query, bias_key, bias_value)
    starts = (0, q_cols, q_cols + HEAD_DIM)
    for start, part in zip(starts, bias):
        span = pl.ds(start, part.shape[1])
        acc[:, span] = jnp.broadcast_to(part[...].astype(F32), (rows, part.shape[1]))

    def project(t, carry):
        ring_advance(w_all, w_sems, t)
        partner_wait(w_all, w_sems, t)
        for d in range(2):
            i = 2 * source_at(d, t, core) + d
            k = 2 * source_at(d, t, 1 - core) + d
            acc[...] += jnp.dot(normed(i), w_all[i], preferred_element_type=F32) + jnp.dot(
                normed(k), w_all[k], preferred_element_type=F32
            )
        return carry

    lax.fori_loop(0, chips, project, 0)

    block_cos, block_sin = far_cos[me], far_sin[me]
    cosine = near_cos[...] * block_cos - near_sin[...] * block_sin
    lane = lax.broadcasted_iota(jnp.int32, cosine.shape, 1)
    sine = near_sin[...] * block_cos + near_cos[...] * block_sin
    sine = jnp.where(lane < HEAD_DIM // 2, -sine, sine)

    def rotary(x):
        return x * cosine + pltpu.roll(x, HEAD_DIM // 2, 1) * sine

    def kv_rows(which):
        return pl.ds(pl.multiple_of(which * rows, rows), rows)

    kv_all[chip, kv_rows(core), pl.ds(0, HEAD_DIM)] = rotary(acc[:, pl.ds(q_cols, HEAD_DIM)]).astype(BF16)
    kv_all[chip, kv_rows(core), pl.ds(HEAD_DIM, HEAD_DIM)] = acc[:, pl.ds(q_cols + HEAD_DIM, HEAD_DIM)].astype(BF16)
    for h in range(heads):
        q_ref[h] = rotary(acc[:, pl.ds(h * HEAD_DIM, HEAD_DIM)]).astype(BF16)

    reach = (chips // 2, chips - 1 - chips // 2)

    parts = 2 if rows % 32 == 0 else 1
    piece_rows = rows // parts

    def kv_copy(owner, ss, rs, direction, step, j, device):
        start = pl.multiple_of((owner % 2) * rows + j * piece_rows, piece_rows)
        block = kv_all.at[owner // 2, pl.ds(start, piece_rows)]
        return remote(block, ss, rs, key_of(direction, step, j), device)

    for j in range(parts):
        for d in range(2):
            kv_copy(me, ks, kr, d, 0, j, neighbours[d]).start()
        kv_copy(me, kps, kpr, 0, chips - 1, j, partner).start()

    factor = HEAD_DIM ** (-0.5) * 1.4426950408889634

    def attend(c, own):
        for h in range(heads):
            scores = lax.dot_general(
                q_ref[h], kv_all[c, :, pl.ds(0, HEAD_DIM)], (((1,), (1,)), ((), ())),
                preferred_element_type=F32,
            )
            if own:
                row = lax.broadcasted_iota(jnp.int32, scores.shape, 0) + core * rows
                col = lax.broadcasted_iota(jnp.int32, scores.shape, 1)
                scores = jnp.where(row >= col, scores, -jnp.inf)
            top = jnp.max(scores, axis=-1, keepdims=True)
            if not own:
                old = high[h]
                top = jnp.maximum(old, top)
            probs = jnp.exp2((scores - top) * factor)
            part = jnp.sum(probs, axis=-1, keepdims=True)
            product = jnp.dot(
                probs.astype(BF16), kv_all[c, :, pl.ds(HEAD_DIM, HEAD_DIM)], preferred_element_type=F32
            )
            if not own:
                shrink = jnp.exp2((old - top) * factor)
                part = part + total[h] * shrink
                product = product + mixed[h] * shrink
            high[h] = top
            total[h] = part
            mixed[h] = product

    for j in range(parts):
        kv_copy(partner, kps, kpr, 0, chips - 1, j, partner).wait_recv()
    attend(chip, True)

    def attention(t, carry):
        for j in range(parts):
            for d in range(2):
                @pl.when(t < reach[d])
                def _():
                    owner = source_at(d, t + 1, core)
                    kv_copy(owner, ks, kr, d, t, j, neighbours[d]).wait_recv()

                    @pl.when(t + 1 < reach[d])
                    def _():
                        kv_copy(owner, ks, kr, d, t + 1, j, neighbours[d]).start()

                    kv_copy(owner, kps, kpr, d, t, j, partner).start()

        @pl.when(t == reach[0])
        def _():
            ring_begin(wo_all, o_sems)

        for d in range(2):
            @pl.when((t > 0) & (t <= reach[d]))
            def _():
                owner = source_at(d, t, 1 - core)
                for j in range(parts):
                    kv_copy(owner, kps, kpr, d, t - 1, j, partner).wait_recv()

                @pl.when(owner // 2 < chip)
                def _():
                    attend(owner // 2, False)
        return carry

    lax.fori_loop(0, reach[0] + 1, attention, 0)
    for h in range(heads):
        att[:, pl.ds(h * HEAD_DIM, HEAD_DIM)] = (mixed[h] / total[h]).astype(BF16)

    def term_copy(p, i):
        return pltpu.make_async_remote_copy(
            src_ref=ts.at[p - 1, i], dst_ref=tr.at[p - 1, i],
            send_sem=ys.at[(p - 1) * slices + i], recv_sem=yr.at[(p - 1) * slices + i],
            device_id={"head": (group + p) % groups}, device_id_type=MESH,
        )

    def out_columns(i):
        return pl.ds(pl.multiple_of(i * half_cols, half_cols), half_cols)

    def make_term(i):
        if not exchange:
            out[:, out_columns(i)] = jnp.dot(att[...], wo_all[i], preferred_element_type=F32).astype(BF16)
            return
        for p in peers:
            span = pl.ds(pl.multiple_of(((group + p) % groups) * rh, rh), rh)
            ts[p - 1, i] = jnp.dot(att[span, :], wo_all[i], preferred_element_type=F32).astype(BF16)
            term_copy(p, i).start()
        span = pl.ds(pl.multiple_of(group * rh, rh), rh)
        tm[i] = jnp.dot(att[span, :], wo_all[i], preferred_element_type=F32).astype(BF16)

    def blocks_of(t):
        return [2 * source_at(d, t, which) + d for d in range(2) for which in (core, 1 - core)]

    def finish(t, carry):
        for i in blocks_of(t):
            value = tm[i].astype(F32)
            for p in peers:
                term_copy(p, i).wait_recv()
                value = value + tr[p - 1, i].astype(F32)
            out[:, out_columns(i)] = value.astype(BF16)
        return carry

    lag = 3

    def project_out(t, carry):
        ring_advance(wo_all, o_sems, t)
        partner_wait(wo_all, o_sems, t)
        for i in blocks_of(t):
            make_term(i)
        if exchange:
            @pl.when(t >= lag)
            def _():
                finish(t - lag, 0)
        return carry

    lax.fori_loop(0, chips, project_out, 0)

    if exchange:
        lax.fori_loop(chips - lag, chips, finish, 0)

        def sent(i, carry):
            for p in peers:
                term_copy(p, i).wait_send()
            return carry

        lax.fori_loop(0, slices, sent, 0)

    ring_drain(w_all, w_sems)
    ring_drain(wo_all, o_sems)
    for j in range(parts):
        for d in range(2):
            for t in range(reach[d]):
                kv_copy(me, ks, kr, d, t, j, neighbours[d]).wait_send()
                kv_copy(me, kps, kpr, d, t, j, partner).wait_send()
        kv_copy(me, kps, kpr, 0, chips - 1, j, partner).wait_send()


def local(n, groups, hidden, norm_gain, w_query, w_key, w_value, bias_query, bias_key, bias_value, w_out):
    rows, width = hidden.shape
    cols = w_query.shape[1]
    heads = cols // HEAD_DIM
    wide = cols + 2 * HEAD_DIM
    chips = n // 2
    exchange = groups > 1 and (rows // groups) % 16 == 0
    rh = rows // groups
    slices = 2 * n
    half_depth = w_query.shape[0] // 2
    half_cols = w_out.shape[1] // 2

    freq = ROPE_BASE ** (-2.0 * np.arange(HEAD_DIM // 2, dtype=np.float64) / HEAD_DIM)
    freq = np.concatenate([freq, freq])
    near = np.arange(rows, dtype=np.float64)[:, None] * freq
    far = (np.arange(n, dtype=np.float64) * rows)[:, None, None] * freq
    tables = [f(a).astype(np.float32) for a in (near, far) for f in (np.cos, np.sin)]
    vectors = [v.reshape(1, -1) for v in (norm_gain, bias_query, bias_key, bias_value)]

    any_spec = pl.BlockSpec(memory_space=pl.ANY)
    vmem = pl.BlockSpec(memory_space=pltpu.VMEM)
    links = max(groups - 1, 1) if exchange else 1
    pieces = slices if exchange else 1
    rpart = rh if exchange else 16
    dma = pltpu.SemaphoreType.DMA
    result = pl.pallas_call(
        functools.partial(kernel, n, groups, exchange),
        out_shape=jax.ShapeDtypeStruct((rh if exchange else rows, w_out.shape[1] * n), BF16),
        in_specs=[any_spec] * 5 + [vmem] * 8,
        out_specs=vmem,
        scratch_shapes=[
            pltpu.VMEM((rows, width), BF16),
            pltpu.VMEM((slices, half_depth, wide), BF16),
            pltpu.VMEM((slices, w_out.shape[0], half_cols), BF16),
            pltpu.VMEM((rows, wide), F32),
            pltpu.VMEM((chips, 2 * rows, 2 * HEAD_DIM), BF16),
            pltpu.VMEM((heads, rows, HEAD_DIM), BF16),
            pltpu.VMEM((heads, rows, 1), F32),
            pltpu.VMEM((heads, rows, 1), F32),
            pltpu.VMEM((heads, rows, HEAD_DIM), F32),
            pltpu.VMEM((rows, cols), BF16),
            pltpu.VMEM((links, pieces, rpart, half_cols), BF16),
            pltpu.VMEM((links, pieces, rpart, half_cols), BF16),
            pltpu.VMEM((pieces, rpart, half_cols), BF16),
            dma((9,)),
        ]
        + [dma((4 * chips,))] * 12
        + [dma((links * pieces,))] * 2,
        compiler_params=pltpu.CompilerParams(
            collective_id=0, has_side_effects=True, vmem_limit_bytes=64 * 1024 * 1024 - 128 * 1024
        ),
    )(hidden, w_query, w_key, w_value, w_out, *vectors, *tables)
    if exchange:
        return result
    return lax.psum_scatter(result, "head", scatter_dimension=0, tiled=True)


def solution(mesh):
    in_specs = (
        P("seq", None),
        P(),
        P("seq", "head"),
        P("seq", "head"),
        P("seq", "head"),
        P("head"),
        P("head"),
        P("head"),
        P("head", "seq"),
    )
    out_specs = P(("seq", "head"), None)
    body = functools.partial(local, mesh.shape["seq"], mesh.shape["head"])
    return jax.shard_map(body, mesh=mesh, in_specs=in_specs, out_specs=out_specs, check_vma=False)
```

```python
import functools

import jax
import jax.numpy as jnp
import numpy as np
from jax import lax
from jax.experimental import pallas as pl
from jax.experimental.pallas import tpu as pltpu
from jax.sharding import PartitionSpec as P

HEAD_DIM = 128
ROPE_BASE = 1000000.0
EPSILON = 1e-06
MESH = pl.DeviceIdType.MESH
F32 = jnp.float32
BF16 = jnp.bfloat16


def kernel(
    n, groups, exchange,
    hidden, w_query, w_key, w_value, w_out, gain, bias_query, bias_key, bias_value,
    near_cos, near_sin, far_cos, far_sin,
    out,
    hid, w_all, wo_all, acc, kv_all, q_ref, high, total, mixed, att, ts, tr, tm,
    load_sem, ws, wr, wps, wpr, os_, or_, ops, opr, ks, kr, kps, kpr, ys, yr,
):
    chips = n // 2
    depth = chips // 2
    me = lax.axis_index("seq")
    group = lax.axis_index("head")
    core = me % 2
    chip = me // 2
    ring = chip // 2 + (chip % 2) * (2 * depth - 1 - 2 * (chip // 2))

    def device_at(position, which):
        position = (position + 2 * chips) % chips
        side = position // depth
        row = position + side * (2 * depth - 1 - 2 * position)
        return 2 * (2 * row + side) + which

    right = device_at(ring + 1, core)
    left = device_at(ring - 1, core)
    partner = 2 * chip + (1 - core)
    neighbours = (right, left)

    def source_at(direction, offset, which):
        return device_at(ring - offset if direction == 0 else ring + offset, which)

    rows, width = hidden.shape
    half_depth = w_query.shape[0] // 2
    q_cols = w_query.shape[1]
    heads = q_cols // HEAD_DIM
    half_cols = w_out.shape[1] // 2
    rh = rows // groups

    loads = []
    late = [pltpu.make_async_copy(hidden, hid, load_sem.at[0])]
    for h in range(2):
        span = pl.ds(h * half_depth, half_depth)
        slot = w_all.at[2 * me + h]
        loads.append(pltpu.make_async_copy(w_query.at[span], slot.at[:, pl.ds(0, q_cols)], load_sem.at[1 + 4 * h]))
        loads.append(pltpu.make_async_copy(w_key.at[span], slot.at[:, pl.ds(q_cols, HEAD_DIM)], load_sem.at[2 + 4 * h]))
        loads.append(pltpu.make_async_copy(w_value.at[span], slot.at[:, pl.ds(q_cols + HEAD_DIM, HEAD_DIM)], load_sem.at[3 + 4 * h]))
        late.append(pltpu.make_async_copy(w_out.at[:, pl.ds(h * half_cols, half_cols)], wo_all.at[2 * me + h], load_sem.at[4 + 4 * h]))
    for copy in loads + late:
        copy.start()

    barrier = pltpu.get_barrier_semaphore()
    for device in (right, left, partner):
        pl.semaphore_signal(barrier, inc=1, device_id={"seq": device}, device_id_type=MESH)
    peers = range(1, groups) if exchange else ()
    for p in peers:
        pl.semaphore_signal(barrier, inc=1, device_id={"head": (group + p) % groups}, device_id_type=MESH)
    pl.semaphore_wait(barrier, 3 + len(peers))

    def remote(ref, send, recv, key, device):
        return pltpu.make_async_remote_copy(
            src_ref=ref, dst_ref=ref, send_sem=send.at[key], recv_sem=recv.at[key],
            device_id={"seq": device}, device_id_type=MESH,
        )

    def piece(buffer, index, j):
        size = buffer.shape[1] // 2
        return buffer.at[index, pl.ds(j * size, size)]

    def key_of(direction, step, j):
        return (direction * chips + step) * 2 + j

    def ring_begin(buffer, sems):
        ss, rs, pss, prs = sems
        for j in range(2):
            for d in range(2):
                own = piece(buffer, 2 * me + d, j)
                remote(own, ss, rs, key_of(d, 0, j), neighbours[d]).start()
        for j in range(2):
            for d in range(2):
                own = piece(buffer, 2 * me + d, j)
                remote(own, pss, prs, key_of(d, chips - 1, j), partner).start()

    def ring_advance(buffer, sems, t):
        ss, rs, pss, prs = sems

        @pl.when(t < chips - 1)
        def _():
            for j in range(2):
                for d in range(2):
                    block = piece(buffer, 2 * source_at(d, t + 1, core) + d, j)
                    remote(block, ss, rs, key_of(d, t, j), neighbours[d]).wait_recv()

                    @pl.when(t < chips - 2)
                    def _():
                        remote(block, ss, rs, key_of(d, t + 1, j), neighbours[d]).start()

                    remote(block, pss, prs, key_of(d, t, j), partner).start()

    def partner_wait(buffer, sems, t):
        ss, rs, pss, prs = sems
        for j in range(2):
            for d in range(2):
                block = piece(buffer, 2 * source_at(d, t, 1 - core) + d, j)
                remote(block, pss, prs, key_of(d, (t + chips - 1) % chips, j), partner).wait_recv()

    def ring_drain(buffer, sems):
        ss, rs, pss, prs = sems

        def body(t, carry):
            for j in range(2):
                for d in range(2):
                    block = piece(buffer, 2 * me + d, j)

                    @pl.when(t < chips - 1)
                    def _():
                        remote(block, ss, rs, key_of(d, t, j), neighbours[d]).wait_send()

                    remote(block, pss, prs, key_of(d, t, j), partner).wait_send()
            return carry

        lax.fori_loop(0, chips, body, 0)

    w_sems = (ws, wr, wps, wpr)
    o_sems = (os_, or_, ops, opr)

    for copy in loads:
        copy.wait()
    ring_begin(w_all, w_sems)
    for copy in late:
        copy.wait()
    slices = 2 * n
    step_cols = width // slices

    def columns(i):
        return pl.ds(pl.multiple_of(i * step_cols, step_cols), step_cols)

    def square(i, carry):
        x = hid[:, columns(i)].astype(F32)
        return carry + x * x

    squares = lax.fori_loop(0, slices, square, jnp.zeros((rows, step_cols), F32))
    inverse = lax.rsqrt(jnp.sum(squares, axis=-1, keepdims=True) * (1.0 / width) + EPSILON)

    def normed(i):
        scaled = hid[:, columns(i)].astype(F32) * inverse * gain[:, columns(i)].astype(F32)
        return scaled.astype(BF16)

    bias = (bias_query, bias_key, bias_value)
    starts = (0, q_cols, q_cols + HEAD_DIM)
    for start, part in zip(starts, bias):
        span = pl.ds(start, part.shape[1])
        acc[:, span] = jnp.broadcast_to(part[...].astype(F32), (rows, part.shape[1]))

    def project(t, carry):
        ring_advance(w_all, w_sems, t)
        partner_wait(w_all, w_sems, t)
        for d in range(2):
            i = 2 * source_at(d, t, core) + d
            k = 2 * source_at(d, t, 1 - core) + d
            acc[...] += jnp.dot(normed(i), w_all[i], preferred_element_type=F32) + jnp.dot(
                normed(k), w_all[k], preferred_element_type=F32
            )
        return carry

    lax.fori_loop(0, chips, project, 0)

    block_cos, block_sin = far_cos[me], far_sin[me]
    cosine = near_cos[...] * block_cos - near_sin[...] * block_sin
    lane = lax.broadcasted_iota(jnp.int32, cosine.shape, 1)
    sine = near_sin[...] * block_cos + near_cos[...] * block_sin
    sine = jnp.where(lane < HEAD_DIM // 2, -sine, sine)

    def rotary(x):
        return x * cosine + pltpu.roll(x, HEAD_DIM // 2, 1) * sine

    def kv_rows(which):
        return pl.ds(pl.multiple_of(which * rows, rows), rows)

    kv_all[chip, kv_rows(core), pl.ds(0, HEAD_DIM)] = rotary(acc[:, pl.ds(q_cols, HEAD_DIM)]).astype(BF16)
    kv_all[chip, kv_rows(core), pl.ds(HEAD_DIM, HEAD_DIM)] = acc[:, pl.ds(q_cols + HEAD_DIM, HEAD_DIM)].astype(BF16)
    for h in range(heads):
        q_ref[h] = rotary(acc[:, pl.ds(h * HEAD_DIM, HEAD_DIM)]).astype(BF16)

    reach = (chips // 2, chips - 1 - chips // 2)

    parts = 2 if rows % 32 == 0 else 1
    piece_rows = rows // parts

    def kv_copy(owner, ss, rs, direction, step, j, device):
        start = pl.multiple_of((owner % 2) * rows + j * piece_rows, piece_rows)
        block = kv_all.at[owner // 2, pl.ds(start, piece_rows)]
        return remote(block, ss, rs, key_of(direction, step, j), device)

    for j in range(parts):
        for d in range(2):
            kv_copy(me, ks, kr, d, 0, j, neighbours[d]).start()
        kv_copy(me, kps, kpr, 0, chips - 1, j, partner).start()

    factor = HEAD_DIM ** (-0.5) * 1.4426950408889634

    def attend(c, own):
        for h in range(heads):
            scores = lax.dot_general(
                q_ref[h], kv_all[c, :, pl.ds(0, HEAD_DIM)], (((1,), (1,)), ((), ())),
                preferred_element_type=F32,
            )
            if own:
                row = lax.broadcasted_iota(jnp.int32, scores.shape, 0) + core * rows
                col = lax.broadcasted_iota(jnp.int32, scores.shape, 1)
                scores = jnp.where(row >= col, scores, -jnp.inf)
            top = jnp.max(scores, axis=-1, keepdims=True)
            if not own:
                old = high[h]
                top = jnp.maximum(old, top)
            probs = jnp.exp2((scores - top) * factor)
            part = jnp.sum(probs, axis=-1, keepdims=True)
            product = jnp.dot(
                probs.astype(BF16), kv_all[c, :, pl.ds(HEAD_DIM, HEAD_DIM)], preferred_element_type=F32
            )
            if not own:
                shrink = jnp.exp2((old - top) * factor)
                part = part + total[h] * shrink
                product = product + mixed[h] * shrink
            high[h] = top
            total[h] = part
            mixed[h] = product

    for j in range(parts):
        kv_copy(partner, kps, kpr, 0, chips - 1, j, partner).wait_recv()
    attend(chip, True)

    def attention(t, carry):
        for j in range(parts):
            for d in range(2):
                @pl.when(t < reach[d])
                def _():
                    owner = source_at(d, t + 1, core)
                    kv_copy(owner, ks, kr, d, t, j, neighbours[d]).wait_recv()

                    @pl.when(t + 1 < reach[d])
                    def _():
                        kv_copy(owner, ks, kr, d, t + 1, j, neighbours[d]).start()

                    kv_copy(owner, kps, kpr, d, t, j, partner).start()

        @pl.when(t == reach[0] - 1)
        def _():
            ring_begin(wo_all, o_sems)

        for d in range(2):
            @pl.when((t > 0) & (t <= reach[d]))
            def _():
                owner = source_at(d, t, 1 - core)
                for j in range(parts):
                    kv_copy(owner, kps, kpr, d, t - 1, j, partner).wait_recv()

                @pl.when(owner // 2 < chip)
                def _():
                    attend(owner // 2, False)
        return carry

    lax.fori_loop(0, reach[0] + 1, attention, 0)
    for h in range(heads):
        att[:, pl.ds(h * HEAD_DIM, HEAD_DIM)] = (mixed[h] / total[h]).astype(BF16)

    def term_copy(p, i):
        return pltpu.make_async_remote_copy(
            src_ref=ts.at[p - 1, i], dst_ref=tr.at[p - 1, i],
            send_sem=ys.at[(p - 1) * slices + i], recv_sem=yr.at[(p - 1) * slices + i],
            device_id={"head": (group + p) % groups}, device_id_type=MESH,
        )

    def out_columns(i):
        return pl.ds(pl.multiple_of(i * half_cols, half_cols), half_cols)

    def make_term(i):
        if not exchange:
            out[:, out_columns(i)] = jnp.dot(att[...], wo_all[i], preferred_element_type=F32).astype(BF16)
            return
        for p in peers:
            span = pl.ds(pl.multiple_of(((group + p) % groups) * rh, rh), rh)
            ts[p - 1, i] = jnp.dot(att[span, :], wo_all[i], preferred_element_type=F32).astype(BF16)
            term_copy(p, i).start()
        span = pl.ds(pl.multiple_of(group * rh, rh), rh)
        tm[i] = jnp.dot(att[span, :], wo_all[i], preferred_element_type=F32).astype(BF16)

    def blocks_of(t):
        return [2 * source_at(d, t, which) + d for d in range(2) for which in (core, 1 - core)]

    def finish(t, carry):
        for i in blocks_of(t):
            value = tm[i].astype(F32)
            for p in peers:
                term_copy(p, i).wait_recv()
                value = value + tr[p - 1, i].astype(F32)
            out[:, out_columns(i)] = value.astype(BF16)
        return carry

    lag = 3

    def partner_terms(t):
        partner_wait(wo_all, o_sems, t)
        for d in range(2):
            make_term(2 * source_at(d, t, 1 - core) + d)

    for d in range(2):
        make_term(2 * me + d)
    partner_terms(0)

    def project_out(t, carry):
        ring_advance(wo_all, o_sems, t)

        @pl.when(t < chips - 1)
        def _():
            for d in range(2):
                make_term(2 * source_at(d, t + 1, core) + d)

        @pl.when(t > 0)
        def _():
            partner_terms(t)

        if exchange:
            @pl.when(t >= lag)
            def _():
                finish(t - lag, 0)
        return carry

    lax.fori_loop(0, chips, project_out, 0)

    if exchange:
        lax.fori_loop(chips - lag, chips, finish, 0)

        def sent(i, carry):
            for p in peers:
                term_copy(p, i).wait_send()
            return carry

        lax.fori_loop(0, slices, sent, 0)

    ring_drain(w_all, w_sems)
    ring_drain(wo_all, o_sems)
    for j in range(parts):
        for d in range(2):
            for t in range(reach[d]):
                kv_copy(me, ks, kr, d, t, j, neighbours[d]).wait_send()
                kv_copy(me, kps, kpr, d, t, j, partner).wait_send()
        kv_copy(me, kps, kpr, 0, chips - 1, j, partner).wait_send()


def local(n, groups, hidden, norm_gain, w_query, w_key, w_value, bias_query, bias_key, bias_value, w_out):
    rows, width = hidden.shape
    cols = w_query.shape[1]
    heads = cols // HEAD_DIM
    wide = cols + 2 * HEAD_DIM
    chips = n // 2
    exchange = groups > 1 and (rows // groups) % 16 == 0
    rh = rows // groups
    slices = 2 * n
    half_depth = w_query.shape[0] // 2
    half_cols = w_out.shape[1] // 2

    freq = ROPE_BASE ** (-2.0 * np.arange(HEAD_DIM // 2, dtype=np.float64) / HEAD_DIM)
    freq = np.concatenate([freq, freq])
    near = np.arange(rows, dtype=np.float64)[:, None] * freq
    far = (np.arange(n, dtype=np.float64) * rows)[:, None, None] * freq
    tables = [f(a).astype(np.float32) for a in (near, far) for f in (np.cos, np.sin)]
    vectors = [v.reshape(1, -1) for v in (norm_gain, bias_query, bias_key, bias_value)]

    any_spec = pl.BlockSpec(memory_space=pl.ANY)
    vmem = pl.BlockSpec(memory_space=pltpu.VMEM)
    links = max(groups - 1, 1) if exchange else 1
    pieces = slices if exchange else 1
    rpart = rh if exchange else 16
    dma = pltpu.SemaphoreType.DMA
    result = pl.pallas_call(
        functools.partial(kernel, n, groups, exchange),
        out_shape=jax.ShapeDtypeStruct((rh if exchange else rows, w_out.shape[1] * n), BF16),
        in_specs=[any_spec] * 5 + [vmem] * 8,
        out_specs=vmem,
        scratch_shapes=[
            pltpu.VMEM((rows, width), BF16),
            pltpu.VMEM((slices, half_depth, wide), BF16),
            pltpu.VMEM((slices, w_out.shape[0], half_cols), BF16),
            pltpu.VMEM((rows, wide), F32),
            pltpu.VMEM((chips, 2 * rows, 2 * HEAD_DIM), BF16),
            pltpu.VMEM((heads, rows, HEAD_DIM), BF16),
            pltpu.VMEM((heads, rows, 1), F32),
            pltpu.VMEM((heads, rows, 1), F32),
            pltpu.VMEM((heads, rows, HEAD_DIM), F32),
            pltpu.VMEM((rows, cols), BF16),
            pltpu.VMEM((links, pieces, rpart, half_cols), BF16),
            pltpu.VMEM((links, pieces, rpart, half_cols), BF16),
            pltpu.VMEM((pieces, rpart, half_cols), BF16),
            dma((9,)),
        ]
        + [dma((4 * chips,))] * 12
        + [dma((links * pieces,))] * 2,
        compiler_params=pltpu.CompilerParams(
            collective_id=0, has_side_effects=True, vmem_limit_bytes=64 * 1024 * 1024 - 128 * 1024
        ),
    )(hidden, w_query, w_key, w_value, w_out, *vectors, *tables)
    if exchange:
        return result
    return lax.psum_scatter(result, "head", scatter_dimension=0, tiled=True)


def solution(mesh):
    in_specs = (
        P("seq", None),
        P(),
        P("seq", "head"),
        P("seq", "head"),
        P("seq", "head"),
        P("head"),
        P("head"),
        P("head"),
        P("head", "seq"),
    )
    out_specs = P(("seq", "head"), None)
    body = functools.partial(local, mesh.shape["seq"], mesh.shape["head"])
    return jax.shard_map(body, mesh=mesh, in_specs=in_specs, out_specs=out_specs, check_vma=False)
```
